32 devices in a mesh: dom: 32 (over z, y, x, core).
Axes of the slice: x: 2, y: 2, z: 4, core: 2. Of those that a mesh axis runs over, the one named last changes fastest.
Arguments:
- node_emb: bfloat16 [16384, 64], P('dom'), may hold values from -6 to 6
- hub_emb: bfloat16 [256, 64], replicated, may hold values from -6 to 6
- tile_vals: bfloat16 [4096, 128, 128], P('dom')
- tile_col: int32 [4096], P('dom'), may hold values from 0 to 5
- tile_dest: int32 [4096], P('dom'), may hold values from 0 to 29, as said below
Outputs:
- node_out: float32 [16384, 64], P('dom')
- hub_out: float32 [256, 64], replicated
The draws below stay inside these ranges and needn't reach their ends.
Inputs may be any that keep to these rules, and one draw needn't show every extreme that they name: tile_dest below 28 names a partition offset from -3 to 3 and a block of that partition; from 28 up it names a hub block. tile_col below 4 names one of the holding partition's own blocks; from 4 up it names a hub block.
All inputs are finite; a program needn't handle non-finite values.
Results may differ from the reference program's by a relative error of at most 0.0003.
Values sent between devices are 32-bit elements.
A program may use at most 64 MiB of HBM per device.

```python
import math
import jax
import jax.numpy as jnp
from jax import lax

TILE = 128
WIDTH = 64
BLK_DEV = 4
TILE_DEV = 128
HUB_BLK = 2
REACH_BITS = 2
LAYERS = 2
SLOTS = 7
NODES = 16384
HUB_ROWS = 256
TILES = 4096
N_DOM = 32


def tile_pair(key):
    seeded = jax.random.fold_in(key, 4711)
    destination = jax.random.randint(jax.random.fold_in(seeded, 1), (TILES,), 0, SLOTS * BLK_DEV + HUB_BLK, dtype=jnp.int32)
    present = jax.random.bernoulli(jax.random.fold_in(seeded, 2), 0.125, (TILES, TILE, TILE))
    weights = jax.random.uniform(jax.random.fold_in(seeded, 3), (TILES, TILE, TILE), jnp.float32, 0.5, 1.5)
    ordinary_scale = 1.0 / math.sqrt(max(1.0, TILE_DEV / BLK_DEV * TILE / 8.0))
    hub_factor = math.sqrt((SLOTS * BLK_DEV + HUB_BLK) / (BLK_DEV * N_DOM))
    scaling = jnp.where(destination >= SLOTS * BLK_DEV, ordinary_scale * hub_factor, ordinary_scale)
    values = present.astype(jnp.float32) * weights * scaling[:, None, None]
    return (destination, values)


def draw_tile_dest(key, part):
    destination, values = tile_pair(key)
    return destination


def draw_tile_vals(key, part):
    destination, values = tile_pair(key)
    return values.astype(jnp.bfloat16)


def with_ends(values, own_key, least, largest):
    dims = values.shape
    index_at = [jax.random.randint(jax.random.fold_in(own_key, axis), (), 0, dims[axis]) for axis in range(len(dims))]
    values = values.at[tuple(index_at)].set(least)
    longest = dims.index(max(dims))
    index_at[longest] = (index_at[longest] + 1) % dims[longest]
    return values.at[tuple(index_at)].set(largest)


def block_scale(rng, dims, pieces, smallest, largest):
    level, own = 1.0, jax.random.fold_in(rng, 6)
    for axis_at, blocks in pieces:
        steps = jnp.exp(jax.random.uniform(jax.random.fold_in(own, axis_at), (blocks,), jnp.float32, smallest / len(pieces), largest / len(pieces)))
        level = level * jnp.repeat(steps, dims[axis_at] // blocks).reshape([-1 if axis == axis_at else 1 for axis in range(len(dims))])
    return level


def normal_values(stream_key, extent, scale, most, split=(), kind=jnp.bfloat16):
    drawn = scale * jax.random.normal(stream_key, extent, jnp.float32)
    if split:
        drawn = drawn * block_scale(stream_key, extent, split, -0.22, 0.18)
    return jnp.clip(drawn, -most, most).astype(kind)


def setup_inputs(seed: int = 0) -> dict:
    keys = jax.random.split(jax.random.key(seed), 6)
    return {
        "node_emb": normal_values(keys[0], (NODES, WIDTH), 1.0, 6.0, ((0, 32),)),
        "hub_emb": normal_values(keys[1], (HUB_ROWS, WIDTH), 1.0, 6.0),
        "tile_vals": draw_tile_vals(jax.random.fold_in(keys[5], 71), 0),
        "tile_col": with_ends(jax.random.randint(keys[3], (TILES,), 0, BLK_DEV + HUB_BLK), jax.random.fold_in(keys[3], 1), 0, (BLK_DEV + HUB_BLK) - 1).astype(jnp.int32),
        "tile_dest": draw_tile_dest(jax.random.fold_in(keys[5], 71), 0),
    }


def propagate(sources_all, tile_vals, tile_col, tile_dest):
    node_blocks = BLK_DEV * N_DOM
    reach_far = 2 ** REACH_BITS - 1
    grouped_vals = tile_vals.reshape(N_DOM, TILE_DEV, TILE, TILE)
    grouped_col = tile_col.reshape(N_DOM, TILE_DEV)
    grouped_dest = tile_dest.reshape(N_DOM, TILE_DEV)

    def one_device(carry, inputs):
        device, values, columns, targets = inputs
        col_block = jnp.where(columns < BLK_DEV, device * BLK_DEV + columns, node_blocks + columns - BLK_DEV).astype(jnp.int32)
        offset = targets // BLK_DEV - reach_far
        peer_part = jnp.mod(device + offset, N_DOM)
        row_block = jnp.where(targets < SLOTS * BLK_DEV, peer_part * BLK_DEV + targets % BLK_DEV, node_blocks + targets - SLOTS * BLK_DEV).astype(jnp.int32)
        picked = sources_all[col_block].astype(jnp.float32)
        products = jnp.einsum("tij,tjd->tid", values.astype(jnp.float32), picked, precision=lax.Precision.HIGHEST)
        return carry.at[row_block].add(products), None

    initial = jnp.zeros((node_blocks + HUB_BLK, TILE, WIDTH), jnp.float32)
    devices = jnp.arange(N_DOM, dtype=jnp.int32)
    result, unused = lax.scan(one_device, initial, (devices, grouped_vals, grouped_col, grouped_dest))
    return result


def reference(node_emb, hub_emb, tile_vals, tile_col, tile_dest):
    node_blocks = BLK_DEV * N_DOM
    layer_zero = jnp.concatenate([node_emb, hub_emb], 0).reshape(node_blocks + HUB_BLK, TILE, WIDTH)
    accumulated = layer_zero.astype(jnp.float32)
    current = layer_zero
    for layer_index in range(LAYERS):
        summed = propagate(current, tile_vals, tile_col, tile_dest)
        accumulated = accumulated + summed
        current = summed.astype(jnp.bfloat16)
    combined = (accumulated / float(LAYERS + 1)).reshape(-1, WIDTH)
    return combined[:NODES], combined[NODES:]
```

```python
import functools
import jax
import jax.numpy as jnp
from jax import lax
from jax.experimental import pallas as pl
from jax.experimental.pallas import tpu as pltpu
from jax.sharding import PartitionSpec as P

REACH_BITS = 2
LAYERS = 2
CHUNKS = 8
GROUP = 4
SUBLANES = 8
MESH = pl.DeviceIdType.MESH


def kernel(
    n, pieces, vals_hbm, col_ref, prev_ref, last_ref, node_ref, hub_ref,
    node_out, hub_out,
    vals, cur, chain, own, hub_own, pair, hub_pair, merged, arrived,
    hub_half, hub_got, hub_all, node_total, hub_total,
    load_sem, pair_send, pair_recv, node_send, node_recv, hub_pair_sem,
    piece_send, piece_recv, cast_send, cast_recv,
):
    me = lax.axis_index("dom")
    parity = lax.rem(me, 2)
    chip = me // 2
    chips = n // 2
    step = 1 - 2 * parity
    partner = me + step
    tiles, tile, _ = vals.shape
    width = node_ref.shape[0]
    own_blocks = node_ref.shape[1] // tile
    hub_blocks = hub_ref.shape[1] // tile
    farthest = 2**REACH_BITS - 1
    slots = 2 * farthest + 1
    half = hub_half.shape[1]
    piece = half // pieces
    stride = chips // pieces
    shift = parity if stride > 1 else 0
    chunk = tiles // load_sem.shape[0]

    def load(c):
        part = pl.ds(c * chunk, chunk)
        return pltpu.make_async_copy(vals_hbm.at[part], vals.at[part], load_sem.at[c])

    for c in range(load_sem.shape[0]):
        load(c).start()

    barrier = pltpu.get_barrier_semaphore()

    def greet(i, _):
        pl.semaphore_signal(barrier, inc=1, device_id=(lax.rem(me + i, n),), device_id_type=MESH)
        return 0

    lax.fori_loop(1, n, greet, 0)

    for b in range(own_blocks):
        block = node_ref[:, b * tile : (b + 1) * tile]
        cur[b] = block
        node_total[b * width : (b + 1) * width] = block.astype(jnp.float32)
    for b in range(hub_blocks):
        block = hub_ref[:, b * tile : (b + 1) * tile]
        cur[own_blocks + b] = block
        hub_total[b * width : (b + 1) * width] = block.astype(jnp.float32)
    chain[tiles] = jnp.zeros((width, tile), jnp.float32)

    def remote(src, dst, send, recv, target):
        return pltpu.make_async_remote_copy(
            src_ref=src, dst_ref=dst, send_sem=send, recv_sem=recv,
            device_id=(target,), device_id_type=MESH,
        )

    def is_owner():
        return lax.rem(chip, stride) == shift

    my_piece = chip // stride
    my_global = parity * pieces + my_piece

    for layer in range(LAYERS):
        def multiply(g, _):
            base = g * GROUP
            parts = [
                lax.dot_general(
                    cur[col_ref[base + u]], vals[base + u], (((1,), (1,)), ((), ())),
                    preferred_element_type=jnp.float32,
                )
                for u in range(GROUP)
            ]
            for u in range(GROUP):
                chain[base + u] = chain[prev_ref[base + u]] + parts[u]
            return 0

        per = chunk // GROUP
        if layer == 0:
            for c in range(load_sem.shape[0]):
                load(c).wait()
                lax.fori_loop(c * per, (c + 1) * per, multiply, 0)
            pl.semaphore_wait(barrier, n - 1)
        else:
            lax.fori_loop(0, tiles // GROUP, multiply, 0)

        for b in range(hub_blocks):
            hub_own[layer, b * width : (b + 1) * width] = chain[last_ref[slots * own_blocks + b]]
        hub_swap = remote(
            hub_own.at[layer, pl.ds(pl.multiple_of((1 - parity) * half, SUBLANES), half)],
            hub_pair.at[layer], hub_pair_sem.at[layer, 0], hub_pair_sem.at[layer, 1], partner,
        )
        hub_swap.start()

        def gather_slot(slot):
            for b in range(own_blocks):
                own[layer, slot, b * width : (b + 1) * width] = chain[last_ref[slot * own_blocks + b]]

        swaps = []
        for i in range(farthest + 1):
            gather_slot(2 * i)
            swap = remote(
                own.at[layer, 2 * i], pair.at[layer, i],
                pair_send.at[layer, i], pair_recv.at[layer, i], partner,
            )
            swap.start()
            swaps.append(swap)
        for i in range(farthest):
            gather_slot(2 * i + 1)

        hub_swap.wait_recv()
        hub_half[layer] = (
            hub_own[layer, pl.ds(pl.multiple_of(parity * half, SUBLANES), half)] + hub_pair[layer]
        )

        def piece_copy(j):
            owner = j * stride + shift
            place = lax.rem(chip - owner + chips, chips)
            return owner, place, remote(
                hub_half.at[layer, pl.ds(j * piece, piece)],
                hub_got.at[layer, jnp.maximum(place - 1, 0)],
                piece_send.at[layer, j], piece_recv.at[layer], 2 * owner + parity,
            )

        for j in range(pieces):
            owner, place, copy = piece_copy(j)

            @pl.when(owner != chip)
            def _():
                copy.start()

        offsets = [m for m in range(1 - farthest, farthest + 2, 2) if m] + [0]
        sends = []
        for i, m in enumerate(offsets):
            index = (step * (m - 1) + farthest) // 2
            remote(
                own.at[layer, 0], pair.at[layer, index],
                pair_send.at[layer, index], pair_recv.at[layer, index], partner,
            ).wait_recv()
            value = pair[layer, index]
            if m <= farthest:
                value = own[layer, farthest + step * m] + value
            merged[layer, i] = value
            if m:
                copy = remote(
                    merged.at[layer, i], arrived.at[layer, i],
                    node_send.at[layer, i], node_recv.at[layer, i],
                    lax.rem(me + step * m + n, n),
                )
                copy.start()
                sends.append(copy)

        def cast_copy(i):
            rows = pl.ds(pl.multiple_of(my_global * piece, SUBLANES), piece)
            return remote(
                hub_all.at[layer, rows], hub_all.at[layer, rows],
                cast_send.at[layer, i - 1], cast_recv.at[layer, my_global], lax.rem(me + i, n),
            )

        @pl.when(is_owner())
        def _():
            pltpu.make_async_copy(hub_got.at[layer], hub_got.at[layer], piece_recv.at[layer]).wait()
            start = pl.multiple_of(my_piece * piece, SUBLANES)
            total = hub_half[layer, pl.ds(start, piece)]
            for i in range(chips - 1):
                total = total + hub_got[layer, i]
            hub_all[layer, pl.ds(pl.multiple_of(my_global * piece, SUBLANES), piece)] = total

            def cast(i, _):
                cast_copy(i).start()
                return 0

            lax.fori_loop(1, n, cast, 0)

        for copy in sends:
            copy.wait_recv()
        for b in range(own_blocks):
            rows = slice(b * width, (b + 1) * width)
            value = merged[layer, len(offsets) - 1, rows]
            for i in range(len(sends)):
                value = value + arrived[layer, i, rows]
            total = node_total[rows] + value
            if layer < LAYERS - 1:
                cur[b] = value.astype(jnp.bfloat16)
                node_total[rows] = total
            else:
                node_out[:, b * tile : (b + 1) * tile] = total / float(LAYERS + 1)

        def land(g):
            rows = pl.ds(g * piece, piece)
            return remote(
                hub_all.at[layer, rows], hub_all.at[layer, rows],
                cast_send.at[layer, 0], cast_recv.at[layer, g], partner,
            )

        for g in range(2 * pieces):
            @pl.when(jnp.logical_not(jnp.logical_and(is_owner(), my_global == g)))
            def _():
                land(g).wait_recv()

        for b in range(hub_blocks):
            rows = slice(b * width, (b + 1) * width)
            value = hub_all[layer, rows]
            total = hub_total[rows] + value
            if layer < LAYERS - 1:
                cur[own_blocks + b] = value.astype(jnp.bfloat16)
                hub_total[rows] = total
            else:
                hub_out[:, b * tile : (b + 1) * tile] = total / float(LAYERS + 1)

        hub_swap.wait_send()
        for copy in swaps + sends:
            copy.wait_send()
        for j in range(pieces):
            owner, place, copy = piece_copy(j)

            @pl.when(owner != chip)
            def _():
                copy.wait_send()

        @pl.when(is_owner())
        def _():
            def done(i, _):
                cast_copy(i).wait_send()
                return 0

            lax.fori_loop(1, n, done, 0)


def shards(n, node_emb, hub_emb, tile_vals, tile_col, tile_dest):
    tiles, tile, _ = tile_vals.shape
    rows, width = node_emb.shape
    hub_rows = hub_emb.shape[0]
    own_blocks, hub_blocks = rows // tile, hub_rows // tile
    farthest = 2**REACH_BITS - 1
    slots = 2 * farthest + 1
    targets = slots * own_blocks + hub_blocks
    half = hub_blocks * width // 2
    chips = n // 2
    pieces = min(half // SUBLANES, chips)
    order = jnp.arange(tiles, dtype=jnp.int32)
    wanted = jnp.concatenate([tile_dest, jnp.arange(targets, dtype=jnp.int32)])
    limit = jnp.concatenate([order, jnp.full((targets,), tiles, jnp.int32)])
    match = (tile_dest[None, :] == wanted[:, None]) & (order[None, :] < limit[:, None])
    found = jnp.max(jnp.where(match, order[None, :], -1), axis=1)
    found = jnp.where(found < 0, tiles, found)
    block = own_blocks * width
    chunks = CHUNKS if tiles % (CHUNKS * GROUP) == 0 else 1
    f32, dma = jnp.float32, pltpu.SemaphoreType.DMA
    vmem = pl.BlockSpec(memory_space=pltpu.VMEM)
    smem = pl.BlockSpec(memory_space=pltpu.SMEM)
    node_out, hub_out = pl.pallas_call(
        functools.partial(kernel, n, pieces),
        out_shape=(
            jax.ShapeDtypeStruct((width, rows), f32),
            jax.ShapeDtypeStruct((width, hub_rows), f32),
        ),
        in_specs=[pl.BlockSpec(memory_space=pl.ANY), smem, smem, smem, vmem, vmem],
        out_specs=(vmem, vmem),
        scratch_shapes=[
            pltpu.VMEM((tiles, tile, tile), jnp.bfloat16),
            pltpu.VMEM((own_blocks + hub_blocks, width, tile), jnp.bfloat16),
            pltpu.VMEM((tiles + 1, width, tile), f32),
            pltpu.VMEM((LAYERS, slots, block, tile), f32),
            pltpu.VMEM((LAYERS, 2 * half, tile), f32),
            pltpu.VMEM((LAYERS, farthest + 1, block, tile), f32),
            pltpu.VMEM((LAYERS, half, tile), f32),
            pltpu.VMEM((LAYERS, farthest + 1, block, tile), f32),
            pltpu.VMEM((LAYERS, farthest, block, tile), f32),
            pltpu.VMEM((LAYERS, half, tile), f32),
            pltpu.VMEM((LAYERS, chips - 1, half // pieces, tile), f32),
            pltpu.VMEM((LAYERS, 2 * half, tile), f32),
            pltpu.VMEM((block, tile), f32),
            pltpu.VMEM((2 * half, tile), f32),
            dma((chunks,)),
            dma((LAYERS, farthest + 1)),
            dma((LAYERS, farthest + 1)),
            dma((LAYERS, farthest)),
            dma((LAYERS, farthest)),
            dma((LAYERS, 2)),
            dma((LAYERS, pieces)),
            dma((LAYERS,)),
            dma((LAYERS, n - 1)),
            dma((LAYERS, 2 * pieces)),
        ],
        compiler_params=pltpu.CompilerParams(collective_id=0, has_side_effects=True),
    )(tile_vals, tile_col, found[:tiles], found[tiles:], node_emb.T, hub_emb.T)
    return node_out.T, hub_out.T


def solution(mesh):
    in_specs = (P("dom", None), P(), P("dom", None, None), P("dom"), P("dom"))
    out_specs = (P("dom", None), P())
    body = functools.partial(shards, mesh.shape["dom"])
    return jax.shard_map(body, mesh=mesh, in_specs=in_specs, out_specs=out_specs, check_vma=False)
```

```python
import functools
import jax
import jax.numpy as jnp
from jax import lax
from jax.experimental import pallas as pl
from jax.experimental.pallas import tpu as pltpu
from jax.sharding import PartitionSpec as P

REACH_BITS = 2
LAYERS = 2
CHUNKS = 8
GROUP = 16
SUBLANES = 8
MESH = pl.DeviceIdType.MESH


def kernel(
    n, pieces, vals_hbm, col_ref, found_ref, node_ref, hub_ref,
    node_out, hub_out,
    vals, cur, chain, own, hub_own, pair, merged, arrived,
    hub_got, hub_all, node_total, hub_total,
    load_sem, pair_send, pair_recv, node_send, node_recv,
    piece_send, piece_recv, cast_send, cast_recv,
):
    me = lax.axis_index("dom")
    parity = lax.rem(me, 2)
    step = 1 - 2 * parity
    partner = me + step
    tiles, tile, _ = vals.shape
    width = node_ref.shape[0]
    own_blocks = node_ref.shape[1] // tile
    hub_blocks = hub_ref.shape[1] // tile
    farthest = 2**REACH_BITS - 1
    slots = 2 * farthest + 1
    piece = hub_own.shape[1] // pieces
    stride = n // pieces
    chunk = tiles // load_sem.shape[0]

    def load(c):
        part = pl.ds(c * chunk, chunk)
        return pltpu.make_async_copy(vals_hbm.at[part], vals.at[part], load_sem.at[c])

    for c in range(load_sem.shape[0]):
        load(c).start()

    barrier = pltpu.get_barrier_semaphore()

    def greet(i, _):
        pl.semaphore_signal(barrier, inc=1, device_id=(lax.rem(me + i, n),), device_id_type=MESH)
        return 0

    lax.fori_loop(1, n, greet, 0)

    for b in range(own_blocks):
        block = node_ref[:, b * tile : (b + 1) * tile]
        cur[b] = block
        node_total[b * width : (b + 1) * width] = block.astype(jnp.float32)
    for b in range(hub_blocks):
        block = hub_ref[:, b * tile : (b + 1) * tile]
        cur[own_blocks + b] = block
        hub_total[b * width : (b + 1) * width] = block.astype(jnp.float32)
    chain[tiles] = jnp.zeros((width, tile), jnp.float32)

    def remote(src, dst, send, recv, target):
        return pltpu.make_async_remote_copy(
            src_ref=src, dst_ref=dst, send_sem=send, recv_sem=recv,
            device_id=(target,), device_id_type=MESH,
        )

    def is_owner():
        return lax.rem(me, stride) == 0

    my_piece = me // stride

    for layer in range(LAYERS):
        def multiply(g, _):
            base = g * GROUP
            parts = [
                lax.dot_general(
                    cur[col_ref[base + u]], vals[base + u], (((1,), (1,)), ((), ())),
                    preferred_element_type=jnp.float32,
                )
                for u in range(GROUP)
            ]
            for u in range(GROUP):
                chain[base + u] = chain[found_ref[base + u]] + parts[u]
            return 0

        per = chunk // GROUP
        if layer == 0:
            for c in range(load_sem.shape[0]):
                load(c).wait()
                lax.fori_loop(c * per, (c + 1) * per, multiply, 0)
            pl.semaphore_wait(barrier, n - 1)
        else:
            lax.fori_loop(0, tiles // GROUP, multiply, 0)

        for b in range(hub_blocks):
            hub_own[layer, b * width : (b + 1) * width] = chain[found_ref[tiles + slots * own_blocks + b]]

        def piece_copy(j):
            owner = j * stride
            place = lax.rem(me - owner + n, n)
            return owner, remote(
                hub_own.at[layer, pl.ds(j * piece, piece)],
                hub_got.at[layer, jnp.maximum(place - 1, 0)],
                piece_send.at[layer, j], piece_recv.at[layer], owner,
            )

        for j in range(pieces):
            owner, copy = piece_copy(j)

            @pl.when(owner != me)
            def _():
                copy.start()

        def gather_slot(slot):
            for b in range(own_blocks):
                own[layer, slot, b * width : (b + 1) * width] = chain[found_ref[tiles + slot * own_blocks + b]]

        swaps = []
        for i in range(farthest + 1):
            gather_slot(2 * i)
            swap = remote(
                own.at[layer, 2 * i], pair.at[layer, i],
                pair_send.at[layer, i], pair_recv.at[layer, i], partner,
            )
            swap.start()
            swaps.append(swap)
        for i in range(farthest):
            gather_slot(2 * i + 1)

        offsets = [m for m in range(1 - farthest, farthest + 2, 2) if m] + [0]
        sends = []
        for i, m in enumerate(offsets):
            index = (step * (m - 1) + farthest) // 2
            remote(
                own.at[layer, 0], pair.at[layer, index],
                pair_send.at[layer, index], pair_recv.at[layer, index], partner,
            ).wait_recv()
            value = pair[layer, index]
            if m <= farthest:
                value = own[layer, farthest + step * m] + value
            merged[layer, i] = value
            if m:
                copy = remote(
                    merged.at[layer, i], arrived.at[layer, i],
                    node_send.at[layer, i], node_recv.at[layer, i],
                    lax.rem(me + step * m + n, n),
                )
                copy.start()
                sends.append(copy)

        def cast_copy(i):
            rows = pl.ds(pl.multiple_of(my_piece * piece, SUBLANES), piece)
            return remote(
                hub_all.at[layer, rows], hub_all.at[layer, rows],
                cast_send.at[layer, i - 1], cast_recv.at[layer, my_piece], lax.rem(me + i, n),
            )

        @pl.when(is_owner())
        def _():
            pltpu.make_async_copy(hub_got.at[layer], hub_got.at[layer], piece_recv.at[layer]).wait()
            start = pl.multiple_of(my_piece * piece, SUBLANES)
            hub_all[layer, pl.ds(start, piece)] = (
                hub_own[layer, pl.ds(start, piece)] + jnp.sum(hub_got[layer], axis=0)
            )

            def cast(i, _):
                cast_copy(i).start()
                return 0

            lax.fori_loop(1, n, cast, 0)

        for copy in sends:
            copy.wait_recv()
        for b in range(own_blocks):
            rows = slice(b * width, (b + 1) * width)
            value = merged[layer, len(offsets) - 1, rows]
            for i in range(len(sends)):
                value = value + arrived[layer, i, rows]
            total = node_total[rows] + value
            if layer < LAYERS - 1:
                cur[b] = value.astype(jnp.bfloat16)
                node_total[rows] = total
            else:
                node_out[:, b * tile : (b + 1) * tile] = total / float(LAYERS + 1)

        def land(g):
            rows = pl.ds(g * piece, piece)
            return remote(
                hub_all.at[layer, rows], hub_all.at[layer, rows],
                cast_send.at[layer, 0], cast_recv.at[layer, g], partner,
            )

        for g in range(pieces):
            @pl.when(jnp.logical_not(jnp.logical_and(is_owner(), my_piece == g)))
            def _():
                land(g).wait_recv()

        for b in range(hub_blocks):
            rows = slice(b * width, (b + 1) * width)
            value = hub_all[layer, rows]
            total = hub_total[rows] + value
            if layer < LAYERS - 1:
                cur[own_blocks + b] = value.astype(jnp.bfloat16)
                hub_total[rows] = total
            else:
                hub_out[:, b * tile : (b + 1) * tile] = total / float(LAYERS + 1)

        for copy in swaps + sends:
            copy.wait_send()
        for j in range(pieces):
            owner, copy = piece_copy(j)

            @pl.when(owner != me)
            def _():
                copy.wait_send()

        @pl.when(is_owner())
        def _():
            def done(i, _):
                cast_copy(i).wait_send()
                return 0

            lax.fori_loop(1, n, done, 0)


def shards(n, node_emb, hub_emb, tile_vals, tile_col, tile_dest):
    tiles, tile, _ = tile_vals.shape
    rows, width = node_emb.shape
    hub_rows = hub_emb.shape[0]
    own_blocks, hub_blocks = rows // tile, hub_rows // tile
    farthest = 2**REACH_BITS - 1
    slots = 2 * farthest + 1
    targets = slots * own_blocks + hub_blocks
    packed = hub_blocks * width
    pieces = min(packed // SUBLANES, n)
    order = jnp.arange(tiles, dtype=jnp.int32)
    wanted = jnp.concatenate([tile_dest, jnp.arange(targets, dtype=jnp.int32)])
    limit = jnp.concatenate([order, jnp.full((targets,), tiles, jnp.int32)])
    match = (tile_dest[None, :] == wanted[:, None]) & (order[None, :] < limit[:, None])
    found = jnp.max(jnp.where(match, order[None, :], -1), axis=1)
    found = jnp.where(found < 0, tiles, found)
    block = own_blocks * width
    chunks = CHUNKS if tiles % (CHUNKS * GROUP) == 0 else 1
    f32, dma = jnp.float32, pltpu.SemaphoreType.DMA
    vmem = pl.BlockSpec(memory_space=pltpu.VMEM)
    smem = pl.BlockSpec(memory_space=pltpu.SMEM)
    node_out, hub_out = pl.pallas_call(
        functools.partial(kernel, n, pieces),
        out_shape=(
            jax.ShapeDtypeStruct((width, rows), f32),
            jax.ShapeDtypeStruct((width, hub_rows), f32),
        ),
        in_specs=[pl.BlockSpec(memory_space=pl.ANY), smem, smem, vmem, vmem],
        out_specs=(vmem, vmem),
        scratch_shapes=[
            pltpu.VMEM((tiles, tile, tile), jnp.bfloat16),
            pltpu.VMEM((own_blocks + hub_blocks, width, tile), jnp.bfloat16),
            pltpu.VMEM((tiles + 1, width, tile), f32),
            pltpu.VMEM((LAYERS, slots, block, tile), f32),
            pltpu.VMEM((LAYERS, packed, tile), f32),
            pltpu.VMEM((LAYERS, farthest + 1, block, tile), f32),
            pltpu.VMEM((LAYERS, farthest + 1, block, tile), f32),
            pltpu.VMEM((LAYERS, farthest, block, tile), f32),
            pltpu.VMEM((LAYERS, n - 1, packed // pieces, tile), f32),
            pltpu.VMEM((LAYERS, packed, tile), f32),
            pltpu.VMEM((block, tile), f32),
            pltpu.VMEM((packed, tile), f32),
            dma((chunks,)),
            dma((LAYERS, farthest + 1)),
            dma((LAYERS, farthest + 1)),
            dma((LAYERS, farthest)),
            dma((LAYERS, farthest)),
            dma((LAYERS, pieces)),
            dma((LAYERS,)),
            dma((LAYERS, n - 1)),
            dma((LAYERS, pieces)),
        ],
        compiler_params=pltpu.CompilerParams(collective_id=0, has_side_effects=True),
    )(tile_vals, tile_col, found, node_emb.T, hub_emb.T)
    return node_out.T, hub_out.T


def solution(mesh):
    in_specs = (P("dom", None), P(), P("dom", None, None), P("dom"), P("dom"))
    out_specs = (P("dom", None), P())
    body = functools.partial(shards, mesh.shape["dom"])
    return jax.shard_map(body, mesh=mesh, in_specs=in_specs, out_specs=out_specs, check_vma=False)
```

```python
import functools
import jax
import jax.numpy as jnp
from jax import lax
from jax.experimental import pallas as pl
from jax.experimental.pallas import tpu as pltpu
from jax.sharding import PartitionSpec as P

REACH_BITS = 2
LAYERS = 2
CHUNKS = 4
GROUP = 32
SUBLANES = 8
MESH = pl.DeviceIdType.MESH


def kernel(
    n, pieces, vals_hbm, col_ref, dest_ref, node_ref, hub_ref,
    node_out, hub_out,
    vals, cur, chain, table, found_ref, own, hub_own, pair, merged, arrived,
    hub_got, hub_all, node_total, hub_total,
    load_sem, table_sem, pair_send, pair_recv, node_send, node_recv,
    piece_send, piece_recv, cast_send, cast_recv,
):
    me = lax.axis_index("dom")
    parity = lax.rem(me, 2)
    step = 1 - 2 * parity
    partner = me + step
    tiles, tile, _ = vals.shape
    width = node_ref.shape[0]
    own_blocks = node_ref.shape[1] // tile
    hub_blocks = hub_ref.shape[1] // tile
    farthest = 2**REACH_BITS - 1
    slots = 2 * farthest + 1
    piece = hub_own.shape[1] // pieces
    stride = n // pieces
    chunk = tiles // load_sem.shape[0]

    def load(c):
        part = pl.ds(c * chunk, chunk)
        return pltpu.make_async_copy(vals_hbm.at[part], vals.at[part], load_sem.at[c])

    for c in range(load_sem.shape[0]):
        load(c).start()

    barrier = pltpu.get_barrier_semaphore()

    def greet(i, _):
        pl.semaphore_signal(barrier, inc=1, device_id=(lax.rem(me + i, n),), device_id_type=MESH)
        return 0

    lax.fori_loop(1, n, greet, 0)

    across = jnp.broadcast_to(dest_ref[...], (tiles, tiles))
    down = across.T
    order = lax.broadcasted_iota(jnp.int32, (tiles, tiles), 0)
    place = lax.broadcasted_iota(jnp.int32, (tiles, tiles), 1)
    earlier = jnp.logical_and(down == across, order < place)
    for i, match in enumerate((earlier, down == place)):
        found = jnp.max(jnp.where(match, order, -1), axis=0, keepdims=True)
        table[i : i + 1] = jnp.where(found < 0, tiles, found)
    table_copy = pltpu.make_async_copy(table, found_ref, table_sem)
    table_copy.start()

    for b in range(own_blocks):
        block = node_ref[:, b * tile : (b + 1) * tile]
        cur[b] = block
        node_total[b * width : (b + 1) * width] = block.astype(jnp.float32)
    for b in range(hub_blocks):
        block = hub_ref[:, b * tile : (b + 1) * tile]
        cur[own_blocks + b] = block
        hub_total[b * width : (b + 1) * width] = block.astype(jnp.float32)
    chain[tiles] = jnp.zeros((width, tile), jnp.float32)
    table_copy.wait()

    def remote(src, dst, send, recv, target):
        return pltpu.make_async_remote_copy(
            src_ref=src, dst_ref=dst, send_sem=send, recv_sem=recv,
            device_id=(target,), device_id_type=MESH,
        )

    def is_owner():
        return lax.rem(me, stride) == 0

    my_piece = me // stride

    for layer in range(LAYERS):
        def multiply(g, _):
            base = g * GROUP
            parts = [
                lax.dot_general(
                    cur[col_ref[base + u]], vals[base + u], (((1,), (1,)), ((), ())),
                    preferred_element_type=jnp.float32,
                )
                for u in range(GROUP)
            ]
            for u in range(GROUP):
                chain[base + u] = chain[found_ref[0, base + u]] + parts[u]
            return 0

        per = chunk // GROUP
        if layer == 0:
            for c in range(load_sem.shape[0]):
                load(c).wait()
                lax.fori_loop(c * per, (c + 1) * per, multiply, 0)
            pl.semaphore_wait(barrier, n - 1)
        else:
            lax.fori_loop(0, tiles // GROUP, multiply, 0)

        for b in range(hub_blocks):
            hub_own[layer, b * width : (b + 1) * width] = chain[found_ref[1, slots * own_blocks + b]]

        def piece_copy(j):
            owner = j * stride
            place = lax.rem(me - owner + n, n)
            return owner, remote(
                hub_own.at[layer, pl.ds(j * piece, piece)],
                hub_got.at[layer, jnp.maximum(place - 1, 0)],
                piece_send.at[layer, j], piece_recv.at[layer], owner,
            )

        for j in range(pieces):
            owner, copy = piece_copy(j)

            @pl.when(owner != me)
            def _():
                copy.start()

        def gather_slot(slot):
            for b in range(own_blocks):
                own[layer, slot, b * width : (b + 1) * width] = chain[found_ref[1, slot * own_blocks + b]]

        swaps = []
        for i in range(farthest + 1):
            gather_slot(2 * i)
            swap = remote(
                own.at[layer, 2 * i], pair.at[layer, i],
                pair_send.at[layer, i], pair_recv.at[layer, i], partner,
            )
            swap.start()
            swaps.append(swap)
        for i in range(farthest):
            gather_slot(2 * i + 1)

        offsets = [m for m in range(1 - farthest, farthest + 2, 2) if m] + [0]
        sends = []
        for i, m in enumerate(offsets):
            index = (step * (m - 1) + farthest) // 2
            remote(
                own.at[layer, 0], pair.at[layer, index],
                pair_send.at[layer, index], pair_recv.at[layer, index], partner,
            ).wait_recv()
            value = pair[layer, index]
            if m <= farthest:
                value = own[layer, farthest + step * m] + value
            merged[layer, i] = value
            if m:
                copy = remote(
                    merged.at[layer, i], arrived.at[layer, i],
                    node_send.at[layer, i], node_recv.at[layer, i],
                    lax.rem(me + step * m + n, n),
                )
                copy.start()
                sends.append(copy)

        def cast_copy(i):
            rows = pl.ds(pl.multiple_of(my_piece * piece, SUBLANES), piece)
            return remote(
                hub_all.at[layer, rows], hub_all.at[layer, rows],
                cast_send.at[layer, i - 1], cast_recv.at[layer, my_piece], lax.rem(me + i, n),
            )

        @pl.when(is_owner())
        def _():
            pltpu.make_async_copy(hub_got.at[layer], hub_got.at[layer], piece_recv.at[layer]).wait()
            start = pl.multiple_of(my_piece * piece, SUBLANES)
            hub_all[layer, pl.ds(start, piece)] = (
                hub_own[layer, pl.ds(start, piece)] + jnp.sum(hub_got[layer], axis=0)
            )

            def cast(i, _):
                cast_copy(i).start()
                return 0

            lax.fori_loop(1, n, cast, 0)

        for copy in sends:
            copy.wait_recv()
        for b in range(own_blocks):
            rows = slice(b * width, (b + 1) * width)
            value = merged[layer, len(offsets) - 1, rows]
            for i in range(len(sends)):
                value = value + arrived[layer, i, rows]
            total = node_total[rows] + value
            if layer < LAYERS - 1:
                cur[b] = value.astype(jnp.bfloat16)
                node_total[rows] = total
            else:
                node_out[:, b * tile : (b + 1) * tile] = total / float(LAYERS + 1)

        def land(g):
            rows = pl.ds(g * piece, piece)
            return remote(
                hub_all.at[layer, rows], hub_all.at[layer, rows],
                cast_send.at[layer, 0], cast_recv.at[layer, g], partner,
            )

        for g in range(pieces):
            @pl.when(jnp.logical_not(jnp.logical_and(is_owner(), my_piece == g)))
            def _():
                land(g).wait_recv()

        for b in range(hub_blocks):
            rows = slice(b * width, (b + 1) * width)
            value = hub_all[layer, rows]
            total = hub_total[rows] + value
            if layer < LAYERS - 1:
                cur[own_blocks + b] = value.astype(jnp.bfloat16)
                hub_total[rows] = total
            else:
                hub_out[:, b * tile : (b + 1) * tile] = total / float(LAYERS + 1)

        for copy in swaps + sends:
            copy.wait_send()
        for j in range(pieces):
            owner, copy = piece_copy(j)

            @pl.when(owner != me)
            def _():
                copy.wait_send()

        @pl.when(is_owner())
        def _():
            def done(i, _):
                cast_copy(i).wait_send()
                return 0

            lax.fori_loop(1, n, done, 0)


def shards(n, node_emb, hub_emb, tile_vals, tile_col, tile_dest):
    tiles, tile, _ = tile_vals.shape
    rows, width = node_emb.shape
    hub_rows = hub_emb.shape[0]
    own_blocks, hub_blocks = rows // tile, hub_rows // tile
    farthest = 2**REACH_BITS - 1
    slots = 2 * farthest + 1
    packed = hub_blocks * width
    pieces = min(packed // SUBLANES, n)
    block = own_blocks * width
    chunks = CHUNKS if tiles % (CHUNKS * GROUP) == 0 else 1
    f32, dma = jnp.float32, pltpu.SemaphoreType.DMA
    vmem = pl.BlockSpec(memory_space=pltpu.VMEM)
    smem = pl.BlockSpec(memory_space=pltpu.SMEM)
    node_out, hub_out = pl.pallas_call(
        functools.partial(kernel, n, pieces),
        out_shape=(
            jax.ShapeDtypeStruct((width, rows), f32),
            jax.ShapeDtypeStruct((width, hub_rows), f32),
        ),
        in_specs=[pl.BlockSpec(memory_space=pl.ANY), smem, vmem, vmem, vmem],
        out_specs=(vmem, vmem),
        scratch_shapes=[
            pltpu.VMEM((tiles, tile, tile), jnp.bfloat16),
            pltpu.VMEM((own_blocks + hub_blocks, width, tile), jnp.bfloat16),
            pltpu.VMEM((tiles + 1, width, tile), f32),
            pltpu.VMEM((2, tiles), jnp.int32),
            pltpu.SMEM((2, tiles), jnp.int32),
            pltpu.VMEM((LAYERS, slots, block, tile), f32),
            pltpu.VMEM((LAYERS, packed, tile), f32),
            pltpu.VMEM((LAYERS, farthest + 1, block, tile), f32),
            pltpu.VMEM((LAYERS, farthest + 1, block, tile), f32),
            pltpu.VMEM((LAYERS, farthest, block, tile), f32),
            pltpu.VMEM((LAYERS, n - 1, packed // pieces, tile), f32),
            pltpu.VMEM((LAYERS, packed, tile), f32),
            pltpu.VMEM((block, tile), f32),
            pltpu.VMEM((packed, tile), f32),
            dma((chunks,)),
            dma,
            dma((LAYERS, farthest + 1)),
            dma((LAYERS, farthest + 1)),
            dma((LAYERS, farthest)),
            dma((LAYERS, farthest)),
            dma((LAYERS, pieces)),
            dma((LAYERS,)),
            dma((LAYERS, n - 1)),
            dma((LAYERS, pieces)),
        ],
        compiler_params=pltpu.CompilerParams(collective_id=0, has_side_effects=True),
    )(tile_vals, tile_col, tile_dest.reshape(1, tiles), node_emb.T, hub_emb.T)
    return node_out.T, hub_out.T


def solution(mesh):
    in_specs = (P("dom", None), P(), P("dom", None, None), P("dom"), P("dom"))
    out_specs = (P("dom", None), P())
    body = functools.partial(shards, mesh.shape["dom"])
    return jax.shard_map(body, mesh=mesh, in_specs=in_specs, out_specs=out_specs, check_vma=False)
```

```python
import functools
import jax
import jax.numpy as jnp
from jax import lax
from jax.experimental import pallas as pl
from jax.experimental.pallas import tpu as pltpu
from jax.sharding import PartitionSpec as P

REACH_BITS = 2
LAYERS = 2
CHUNKS = 4
GROUP = 32
SUBLANES = 8
MESH = pl.DeviceIdType.MESH


def kernel(
    n, pieces, vals_hbm, col_ref, dest_ref, node_ref, hub_ref,
    node_out, hub_out,
    vals, cur, chain, table, found_ref, own, hub_own, pair, merged, arrived,
    hub_got, hub_all, node_total, hub_total,
    load_sem, table_sem, pair_send, pair_recv, node_send, node_recv,
    piece_send, piece_recv, cast_send, cast_recv,
):
    me = lax.axis_index("dom")
    parity = lax.rem(me, 2)
    step = 1 - 2 * parity
    partner = me + step
    tiles, tile, _ = vals.shape
    width = node_ref.shape[0]
    own_blocks = node_ref.shape[1] // tile
    hub_blocks = hub_ref.shape[1] // tile
    farthest = 2**REACH_BITS - 1
    slots = 2 * farthest + 1
    piece = hub_own.shape[1] // pieces
    stride = n // pieces
    chunk = tiles // load_sem.shape[0]

    def load(c):
        part = pl.ds(c * chunk, chunk)
        return pltpu.make_async_copy(vals_hbm.at[part], vals.at[part], load_sem.at[c])

    for c in range(load_sem.shape[0]):
        load(c).start()

    barrier = pltpu.get_barrier_semaphore()

    def greet(i, _):
        pl.semaphore_signal(barrier, inc=1, device_id=(lax.rem(me + i, n),), device_id_type=MESH)
        return 0

    lax.fori_loop(1, n, greet, 0)

    across = jnp.broadcast_to(dest_ref[...], (tiles, tiles))
    down = across.T
    order = lax.broadcasted_iota(jnp.int32, (tiles, tiles), 0)
    place = lax.broadcasted_iota(jnp.int32, (tiles, tiles), 1)
    earlier = jnp.logical_and(down == across, order < place)
    for i, match in enumerate((earlier, down == place)):
        found = jnp.max(jnp.where(match, order, -1), axis=0, keepdims=True)
        table[i : i + 1] = jnp.where(found < 0, tiles, found)
    table_copy = pltpu.make_async_copy(table, found_ref, table_sem)
    table_copy.start()

    for b in range(own_blocks):
        block = node_ref[:, b * tile : (b + 1) * tile]
        cur[b] = block
        node_total[b * width : (b + 1) * width] = block.astype(jnp.float32)
    for b in range(hub_blocks):
        block = hub_ref[:, b * tile : (b + 1) * tile]
        cur[own_blocks + b] = block
        hub_total[b * width : (b + 1) * width] = block.astype(jnp.float32)
    chain[tiles] = jnp.zeros((width, tile), jnp.float32)
    table_copy.wait()

    def remote(src, dst, send, recv, target):
        return pltpu.make_async_remote_copy(
            src_ref=src, dst_ref=dst, send_sem=send, recv_sem=recv,
            device_id=(target,), device_id_type=MESH,
        )

    def is_owner():
        return lax.rem(me, stride) == 0

    my_piece = me // stride

    for layer in range(LAYERS):
        def multiply(g, _):
            base = g * GROUP
            parts = [
                lax.dot_general(
                    cur[col_ref[base + u]], vals[base + u], (((1,), (1,)), ((), ())),
                    preferred_element_type=jnp.float32,
                )
                for u in range(GROUP)
            ]
            for u in range(GROUP):
                chain[base + u] = chain[found_ref[0, base + u]] + parts[u]
            return 0

        per = chunk // GROUP
        if layer == 0:
            for c in range(load_sem.shape[0]):
                load(c).wait()
                lax.fori_loop(c * per, (c + 1) * per, multiply, 0)
            pl.semaphore_wait(barrier, n - 1)
        else:
            lax.fori_loop(0, tiles // GROUP, multiply, 0)

        for b in range(hub_blocks):
            hub_own[layer, b * width : (b + 1) * width] = chain[found_ref[1, slots * own_blocks + b]]

        def piece_copy(j):
            owner = j * stride
            place = lax.rem(me - owner + n, n)
            return owner, remote(
                hub_own.at[layer, pl.ds(j * piece, piece)],
                hub_got.at[layer, jnp.maximum(place - 1, 0)],
                piece_send.at[layer, j], piece_recv.at[layer], owner,
            )

        for j in range(pieces):
            owner, copy = piece_copy(j)

            @pl.when(owner != me)
            def _():
                copy.start()

        def gather_slot(slot):
            for b in range(own_blocks):
                own[layer, slot, b * width : (b + 1) * width] = chain[found_ref[1, slot * own_blocks + b]]

        swaps = []
        for i in range(farthest + 1):
            gather_slot(2 * i)
            swap = remote(
                own.at[layer, 2 * i], pair.at[layer, i],
                pair_send.at[layer, i], pair_recv.at[layer, i], partner,
            )
            swap.start()
            swaps.append(swap)
        for i in range(farthest):
            gather_slot(2 * i + 1)

        offsets = [m for m in range(1 - farthest, farthest + 2, 2) if m] + [0]
        sends = []
        for i, m in enumerate(offsets):
            index = (step * (m - 1) + farthest) // 2
            remote(
                own.at[layer, 0], pair.at[layer, index],
                pair_send.at[layer, index], pair_recv.at[layer, index], partner,
            ).wait_recv()
            value = pair[layer, index]
            if m <= farthest:
                value = own[layer, farthest + step * m] + value
            merged[layer, i] = value
            if m:
                copy = remote(
                    merged.at[layer, i], arrived.at[layer, i],
                    node_send.at[layer, i], node_recv.at[layer, i],
                    lax.rem(me + step * m + n, n),
                )
                copy.start()
                sends.append(copy)

        def cast_copy(i):
            rows = pl.ds(pl.multiple_of(my_piece * piece, SUBLANES), piece)
            return remote(
                hub_all.at[layer, rows], hub_all.at[layer, rows],
                cast_send.at[layer, i - 1], cast_recv.at[layer, my_piece], lax.rem(me + i, n),
            )

        @pl.when(is_owner())
        def _():
            pltpu.make_async_copy(hub_got.at[layer], hub_got.at[layer], piece_recv.at[layer]).wait()
            start = pl.multiple_of(my_piece * piece, SUBLANES)
            hub_all[layer, pl.ds(start, piece)] = (
                hub_own[layer, pl.ds(start, piece)] + jnp.sum(hub_got[layer], axis=0)
            )

            def cast(i, _):
                cast_copy(i).start()
                return 0

            lax.fori_loop(1, n, cast, 0)

        for copy in sends:
            copy.wait_recv()
        for b in range(own_blocks):
            rows = slice(b * width, (b + 1) * width)
            value = merged[layer, len(offsets) - 1, rows]
            for i in range(len(sends)):
                value = value + arrived[layer, i, rows]
            total = node_total[rows] + value
            if layer < LAYERS - 1:
                cur[b] = value.astype(jnp.bfloat16)
                node_total[rows] = total
            else:
                node_out[:, b * tile : (b + 1) * tile] = total / float(LAYERS + 1)

        def land(g):
            rows = pl.ds(g * piece, piece)
            return remote(
                hub_all.at[layer, rows], hub_all.at[layer, rows],
                cast_send.at[layer, 0], cast_recv.at[layer, g], partner,
            )

        for g in range(pieces):
            @pl.when(jnp.logical_not(jnp.logical_and(is_owner(), my_piece == g)))
            def _():
                land(g).wait_recv()

        for b in range(hub_blocks):
            rows = slice(b * width, (b + 1) * width)
            value = hub_all[layer, rows]
            total = hub_total[rows] + value
            if layer < LAYERS - 1:
                cur[own_blocks + b] = value.astype(jnp.bfloat16)
                hub_total[rows] = total
            else:
                hub_out[:, b * tile : (b + 1) * tile] = total / float(LAYERS + 1)

        for copy in swaps + sends:
            copy.wait_send()
        for j in range(pieces):
            owner, copy = piece_copy(j)

            @pl.when(owner != me)
            def _():
                copy.wait_send()

        @pl.when(is_owner())
        def _():
            def done(i, _):
                cast_copy(i).wait_send()
                return 0

            lax.fori_loop(1, n, done, 0)


def shards(n, node_emb, hub_emb, tile_vals, tile_col, tile_dest):
    tiles, tile, _ = tile_vals.shape
    rows, width = node_emb.shape
    hub_rows = hub_emb.shape[0]
    own_blocks, hub_blocks = rows // tile, hub_rows // tile
    farthest = 2**REACH_BITS - 1
    slots = 2 * farthest + 1
    packed = hub_blocks * width
    pieces = min(packed // SUBLANES, n)
    block = own_blocks * width
    chunks = CHUNKS if tiles % (CHUNKS * GROUP) == 0 else 1
    f32, dma = jnp.float32, pltpu.SemaphoreType.DMA
    vmem = pl.BlockSpec(memory_space=pltpu.VMEM)
    smem = pl.BlockSpec(memory_space=pltpu.SMEM)
    node_out, hub_out = pl.pallas_call(
        functools.partial(kernel, n, pieces),
        out_shape=(
            jax.ShapeDtypeStruct((width, rows), f32),
            jax.ShapeDtypeStruct((width, hub_rows), f32),
        ),
        in_specs=[pl.BlockSpec(memory_space=pl.ANY), smem, vmem, vmem, vmem],
        out_specs=(vmem, vmem),
        scratch_shapes=[
            pltpu.VMEM((tiles, tile, tile), jnp.bfloat16),
            pltpu.VMEM((own_blocks + hub_blocks, width, tile), jnp.bfloat16),
            pltpu.VMEM((tiles + 1, width, tile), f32),
            pltpu.VMEM((2, tiles), jnp.int32),
            pltpu.SMEM((2, tiles), jnp.int32),
            pltpu.VMEM((LAYERS, slots, block, tile), f32),
            pltpu.VMEM((LAYERS, packed, tile), f32),
            pltpu.VMEM((LAYERS, farthest + 1, block, tile), f32),
            pltpu.VMEM((LAYERS, farthest + 1, block, tile), f32),
            pltpu.VMEM((LAYERS, farthest, block, tile), f32),
            pltpu.VMEM((LAYERS, n - 1, packed // pieces, tile), f32),
            pltpu.VMEM((LAYERS, packed, tile), f32),
            pltpu.VMEM((block, tile), f32),
            pltpu.VMEM((packed, tile), f32),
            dma((chunks,)),
            dma,
            dma((LAYERS, farthest + 1)),
            dma((LAYERS, farthest + 1)),
            dma((LAYERS, farthest)),
            dma((LAYERS, farthest)),
            dma((LAYERS, pieces)),
            dma((LAYERS,)),
            dma((LAYERS, n - 1)),
            dma((LAYERS, pieces)),
        ],
        compiler_params=pltpu.CompilerParams(collective_id=0, has_side_effects=True, vmem_limit_bytes=52 * 2**20),
    )(tile_vals, tile_col, tile_dest.reshape(1, tiles), node_emb.T, hub_emb.T)
    return node_out.T, hub_out.T


def solution(mesh):
    in_specs = (P("dom", None), P(), P("dom", None, None), P("dom"), P("dom"))
    out_specs = (P("dom", None), P())
    body = functools.partial(shards, mesh.shape["dom"])
    return jax.shard_map(body, mesh=mesh, in_specs=in_specs, out_specs=out_specs, check_vma=False)
```

```python
import functools
import jax
import jax.numpy as jnp
from jax import lax
from jax.experimental import pallas as pl
from jax.experimental.pallas import tpu as pltpu
from jax.sharding import PartitionSpec as P

REACH_BITS = 2
LAYERS = 2
CHUNKS = 4
GROUP = 32
SUBLANES = 8
MESH = pl.DeviceIdType.MESH


def kernel(
    n, pieces, vals_hbm, col_ref, dest_ref, node_ref, hub_ref,
    node_out, hub_out,
    vals, cur, chain, table, found_ref, own, hub_own, pair, merged, arrived,
    hub_got, hub_all, node_total, hub_total,
    load_sem, table_sem, pair_send, pair_recv, node_send, node_recv,
    piece_send, piece_recv, cast_send, cast_recv,
):
    me = lax.axis_index("dom")
    parity = lax.rem(me, 2)
    step = 1 - 2 * parity
    partner = me + step
    tiles, tile, _ = vals.shape
    width = node_ref.shape[0]
    own_blocks = node_ref.shape[1] // tile
    hub_blocks = hub_ref.shape[1] // tile
    farthest = 2**REACH_BITS - 1
    slots = 2 * farthest + 1
    piece = hub_own.shape[1] // pieces
    stride = n // pieces
    chunk = tiles // load_sem.shape[0]

    def load(c):
        part = pl.ds(c * chunk, chunk)
        return pltpu.make_async_copy(vals_hbm.at[part], vals.at[part], load_sem.at[c])

    for c in range(load_sem.shape[0]):
        load(c).start()

    barrier = pltpu.get_barrier_semaphore()

    def greet(i, _):
        pl.semaphore_signal(barrier, inc=1, device_id=(lax.rem(me + i, n),), device_id_type=MESH)
        return 0

    lax.fori_loop(1, n, greet, 0)

    across = jnp.broadcast_to(dest_ref[...], (tiles, tiles))
    down = across.T
    order = lax.broadcasted_iota(jnp.int32, (tiles, tiles), 0)
    place = lax.broadcasted_iota(jnp.int32, (tiles, tiles), 1)
    earlier = jnp.logical_and(down == across, order < place)
    for i, match in enumerate((earlier, down == place)):
        found = jnp.max(jnp.where(match, order, -1), axis=0, keepdims=True)
        table[i : i + 1] = jnp.where(found < 0, tiles, found)
    table_copy = pltpu.make_async_copy(table, found_ref, table_sem)
    table_copy.start()

    for b in range(own_blocks):
        block = node_ref[:, b * tile : (b + 1) * tile]
        cur[b] = block
        node_total[b * width : (b + 1) * width] = block.astype(jnp.float32)
    for b in range(hub_blocks):
        block = hub_ref[:, b * tile : (b + 1) * tile]
        cur[own_blocks + b] = block
        hub_total[b * width : (b + 1) * width] = block.astype(jnp.float32)
    chain[tiles] = jnp.zeros((width, tile), jnp.float32)
    table_copy.wait()

    def remote(src, dst, send, recv, target):
        return pltpu.make_async_remote_copy(
            src_ref=src, dst_ref=dst, send_sem=send, recv_sem=recv,
            device_id=(target,), device_id_type=MESH,
        )

    def is_owner():
        return lax.rem(me, stride) == 0

    my_piece = me // stride

    for layer in range(LAYERS):
        def multiply(g, _):
            base = g * GROUP
            parts = [
                lax.dot_general(
                    cur[col_ref[base + u]], vals[base + u], (((1,), (1,)), ((), ())),
                    preferred_element_type=jnp.float32,
                )
                for u in range(GROUP)
            ]
            for u in range(GROUP):
                chain[base + u] = chain[found_ref[0, base + u]] + parts[u]
            return 0

        per = chunk // GROUP
        if layer == 0:
            for c in range(load_sem.shape[0]):
                load(c).wait()
                lax.fori_loop(c * per, (c + 1) * per, multiply, 0)
            pl.semaphore_wait(barrier, n - 1)
        else:
            lax.fori_loop(0, tiles // GROUP, multiply, 0)

        for b in range(hub_blocks):
            hub_own[layer, b * width : (b + 1) * width] = chain[found_ref[1, slots * own_blocks + b]]

        def piece_copy(j):
            owner = j * stride
            place = lax.rem(me - owner + n, n)
            return owner, remote(
                hub_own.at[layer, pl.ds(j * piece, piece)],
                hub_got.at[layer, jnp.maximum(place - 1, 0)],
                piece_send.at[layer, j], piece_recv.at[layer], owner,
            )

        for j in range(pieces):
            owner, copy = piece_copy(j)

            @pl.when(owner != me)
            def _():
                copy.start()

        def gather_slot(slot):
            for b in range(own_blocks):
                own[layer, slot, b * width : (b + 1) * width] = chain[found_ref[1, slot * own_blocks + b]]

        offsets = [m for m in range(1 - farthest, farthest + 2, 2) if m] + [0]
        swaps = []
        for m in offsets:
            first = (m - 1 + farthest) // 2
            i = parity * first + (1 - parity) * (farthest - first)
            gather_slot(2 * i)
            swap = remote(
                own.at[layer, 2 * i], pair.at[layer, i],
                pair_send.at[layer, i], pair_recv.at[layer, i], partner,
            )
            swap.start()
            swaps.append(swap)
        for i in range(farthest):
            gather_slot(2 * i + 1)

        sends = []
        for i, m in enumerate(offsets):
            index = (step * (m - 1) + farthest) // 2
            remote(
                own.at[layer, 0], pair.at[layer, index],
                pair_send.at[layer, index], pair_recv.at[layer, index], partner,
            ).wait_recv()
            value = pair[layer, index]
            if m <= farthest:
                value = own[layer, farthest + step * m] + value
            merged[layer, i] = value
            if m:
                copy = remote(
                    merged.at[layer, i], arrived.at[layer, i],
                    node_send.at[layer, i], node_recv.at[layer, i],
                    lax.rem(me + step * m + n, n),
                )
                copy.start()
                sends.append(copy)

        def cast_copy(i):
            rows = pl.ds(pl.multiple_of(my_piece * piece, SUBLANES), piece)
            return remote(
                hub_all.at[layer, rows], hub_all.at[layer, rows],
                cast_send.at[layer, i - 1], cast_recv.at[layer, my_piece], lax.rem(me + i, n),
            )

        @pl.when(is_owner())
        def _():
            pltpu.make_async_copy(hub_got.at[layer], hub_got.at[layer], piece_recv.at[layer]).wait()
            start = pl.multiple_of(my_piece * piece, SUBLANES)
            hub_all[layer, pl.ds(start, piece)] = (
                hub_own[layer, pl.ds(start, piece)] + jnp.sum(hub_got[layer], axis=0)
            )

            def cast(i, _):
                cast_copy(i).start()
                return 0

            lax.fori_loop(1, n, cast, 0)

        for copy in sends:
            copy.wait_recv()
        for b in range(own_blocks):
            rows = slice(b * width, (b + 1) * width)
            value = merged[layer, len(offsets) - 1, rows]
            for i in range(len(sends)):
                value = value + arrived[layer, i, rows]
            total = node_total[rows] + value
            if layer < LAYERS - 1:
                cur[b] = value.astype(jnp.bfloat16)
                node_total[rows] = total
            else:
                node_out[:, b * tile : (b + 1) * tile] = total / float(LAYERS + 1)

        def land(g):
            rows = pl.ds(g * piece, piece)
            return remote(
                hub_all.at[layer, rows], hub_all.at[layer, rows],
                cast_send.at[layer, 0], cast_recv.at[layer, g], partner,
            )

        for g in range(pieces):
            @pl.when(jnp.logical_not(jnp.logical_and(is_owner(), my_piece == g)))
            def _():
                land(g).wait_recv()

        for b in range(hub_blocks):
            rows = slice(b * width, (b + 1) * width)
            value = hub_all[layer, rows]
            total = hub_total[rows] + value
            if layer < LAYERS - 1:
                cur[own_blocks + b] = value.astype(jnp.bfloat16)
                hub_total[rows] = total
            else:
                hub_out[:, b * tile : (b + 1) * tile] = total / float(LAYERS + 1)

        for copy in swaps + sends:
            copy.wait_send()
        for j in range(pieces):
            owner, copy = piece_copy(j)

            @pl.when(owner != me)
            def _():
                copy.wait_send()

        @pl.when(is_owner())
        def _():
            def done(i, _):
                cast_copy(i).wait_send()
                return 0

            lax.fori_loop(1, n, done, 0)


def shards(n, node_emb, hub_emb, tile_vals, tile_col, tile_dest):
    tiles, tile, _ = tile_vals.shape
    rows, width = node_emb.shape
    hub_rows = hub_emb.shape[0]
    own_blocks, hub_blocks = rows // tile, hub_rows // tile
    farthest = 2**REACH_BITS - 1
    slots = 2 * farthest + 1
    packed = hub_blocks * width
    pieces = min(packed // SUBLANES, n)
    block = own_blocks * width
    chunks = CHUNKS if tiles % (CHUNKS * GROUP) == 0 else 1
    f32, dma = jnp.float32, pltpu.SemaphoreType.DMA
    vmem = pl.BlockSpec(memory_space=pltpu.VMEM)
    smem = pl.BlockSpec(memory_space=pltpu.SMEM)
    node_out, hub_out = pl.pallas_call(
        functools.partial(kernel, n, pieces),
        out_shape=(
            jax.ShapeDtypeStruct((width, rows), f32),
            jax.ShapeDtypeStruct((width, hub_rows), f32),
        ),
        in_specs=[pl.BlockSpec(memory_space=pl.ANY), smem, vmem, vmem, vmem],
        out_specs=(vmem, vmem),
        scratch_shapes=[
            pltpu.VMEM((tiles, tile, tile), jnp.bfloat16),
            pltpu.VMEM((own_blocks + hub_blocks, width, tile), jnp.bfloat16),
            pltpu.VMEM((tiles + 1, width, tile), f32),
            pltpu.VMEM((2, tiles), jnp.int32),
            pltpu.SMEM((2, tiles), jnp.int32),
            pltpu.VMEM((LAYERS, slots, block, tile), f32),
            pltpu.VMEM((LAYERS, packed, tile), f32),
            pltpu.VMEM((LAYERS, farthest + 1, block, tile), f32),
            pltpu.VMEM((LAYERS, farthest + 1, block, tile), f32),
            pltpu.VMEM((LAYERS, farthest, block, tile), f32),
            pltpu.VMEM((LAYERS, n - 1, packed // pieces, tile), f32),
            pltpu.VMEM((LAYERS, packed, tile), f32),
            pltpu.VMEM((block, tile), f32),
            pltpu.VMEM((packed, tile), f32),
            dma((chunks,)),
            dma,
            dma((LAYERS, farthest + 1)),
            dma((LAYERS, farthest + 1)),
            dma((LAYERS, farthest)),
            dma((LAYERS, farthest)),
            dma((LAYERS, pieces)),
            dma((LAYERS,)),
            dma((LAYERS, n - 1)),
            dma((LAYERS, pieces)),
        ],
        compiler_params=pltpu.CompilerParams(collective_id=0, has_side_effects=True),
    )(tile_vals, tile_col, tile_dest.reshape(1, tiles), node_emb.T, hub_emb.T)
    return node_out.T, hub_out.T


def solution(mesh):
    in_specs = (P("dom", None), P(), P("dom", None, None), P("dom"), P("dom"))
    out_specs = (P("dom", None), P())
    body = functools.partial(shards, mesh.shape["dom"])
    return jax.shard_map(body, mesh=mesh, in_specs=in_specs, out_specs=out_specs, check_vma=False)
```
